128 devices in a mesh: ctx: 16 (over y_hi, z, core), vocab: 8 (over x, y_lo).
Axes of the slice: x: 4, y: 4 (y_hi: 2, y_lo: 2; y = y_hi * 2 + y_lo), z: 4, core: 2. Of those that a mesh axis runs over, the one named last changes fastest.
Arguments:
- hidden_in: bfloat16 [2048, 4096], P('ctx'), may hold values from -128 to 128
- attn_gain: float32 [4096], replicated, may hold values from 0.1 to 1.9
- w_query: bfloat16 [4096, 4096], P(None, 'vocab'), may hold values from -2 to 2
- w_key: bfloat16 [4096, 1024], P(None, 'vocab'), may hold values from -2 to 2
- w_value: bfloat16 [4096, 1024], P(None, 'vocab'), may hold values from -0.09375 to 0.09375
- w_out: bfloat16 [4096, 4096], P('vocab'), may hold values from -0.5 to 0.5
- final_gain: float32 [4096], replicated, may hold values from 0.5 to 1.5
- teacher_head: bfloat16 [65536, 4096], P(('vocab', 'ctx')), may hold values from -18 to 18
- draft_rows: bfloat16 [2048, 2048], P('ctx'), may hold values from -1.5 to 1.5
- draft_head: bfloat16 [65536, 2048], P(('vocab', 'ctx')), may hold values from -64 to 64
- target_ids: int32 [2048], replicated, may hold values from 0 to 65535
- rollout_lengths: int32 [4], replicated, may hold values from 1 to 1024, 2048 in all
- stretch_order: int32 [32], replicated, may hold values from 0 to 31, as said below
Outputs:
- draft_grad: float32 [2048, 2048], P('ctx', 'vocab')
The draws below stay inside these ranges and needn't reach their ends.
Inputs may be any that keep to these rules, and one draw needn't show every extreme that they name: `rollout_lengths`: the lengths add up to 2048. `stretch_order`: each block number appears once; entries 2c and 2c + 1 add up to 31.
All inputs are finite; a program needn't handle non-finite values.
Results may differ from the reference program's by a relative error of at most 0.0045.
Values may be sent and summed in bfloat16 or wider, within the bound.
No kernel may reach another device: no remote copies, remote signals or barrier semaphores. Data moves between devices by JAX's collectives and lax.ppermute only.
A program may use at most 128 MiB of HBM per device.

```python
import math
import jax
import jax.numpy as jnp
import numpy as np
from jax import lax

D = 4096
HEADS = 32
KV_HEADS = 8
HEAD_DIM = 128
DD = 2048
VOCAB = 65536
ROLLOUTS = 4
TOK_DEV = 128
TOKENS = 2048
STRETCHES = 32
N_CTX = 16


def draw_hidden_in(key, part):
    column_scale = 1.0 + 2.0 * jnp.arange(D, dtype=jnp.float32) / (D - 1)
    values = jnp.clip(jax.random.normal(jax.random.fold_in(key, 4), (TOKENS, D), jnp.float32), -6.0, 6.0) * column_scale[None, :]
    return values.astype(jnp.bfloat16)


def draw_w_query(key, part):
    values = jnp.clip(jax.random.normal(jax.random.fold_in(key, 5), (D, HEADS * HEAD_DIM), jnp.float32), -6.0, 6.0) / math.sqrt(D)
    return jnp.clip(values, -2.0, 2.0).astype(jnp.bfloat16)


def draw_w_key(key, part):
    values = jnp.clip(jax.random.normal(jax.random.fold_in(key, 6), (D, KV_HEADS * HEAD_DIM), jnp.float32), -6.0, 6.0) / math.sqrt(D)
    return jnp.clip(values, -2.0, 2.0).astype(jnp.bfloat16)


def boosted_rows(key, rows, width, spread, limit):
    values = jnp.clip(jax.random.normal(jax.random.fold_in(key, 7), (rows, width), jnp.float32), -6.0, 6.0) * spread
    return jnp.clip(values, -limit, limit).astype(jnp.bfloat16)


def draw_teacher_head(key, part):
    return boosted_rows(key, VOCAB, D, 3.0 / math.sqrt(D), 18.0)


def draw_draft_head(key, part):
    return boosted_rows(jax.random.fold_in(key, 13), VOCAB, DD, 12.0 / math.sqrt(DD), 64.0)


def draw_stretch_order(key, part):
    pair_count = STRETCHES // 2
    order = jax.random.permutation(jax.random.fold_in(key, 11), pair_count).astype(jnp.int32)
    flips = jax.random.randint(jax.random.fold_in(key, 12), (pair_count,), 0, 2)
    leading = jnp.where(flips == 1, STRETCHES - 1 - order, order)
    trailing = STRETCHES - 1 - leading
    return jnp.stack([leading, trailing], axis=1).reshape(STRETCHES).astype(jnp.int32)


def set_ends(result, key, least, high):
    longest = result.shape.index(max(result.shape))
    spots = []
    for shift in (0, 1):
        where = [jax.random.randint(jax.random.fold_in(key, axis), (), 0, length) for axis, length in enumerate(result.shape)]
        where[longest] = (where[longest] + shift) % result.shape[longest]
        spots.append(tuple(where))
    return result.at[spots[0]].set(least).at[spots[1]].set(high)


def shard_levels(rng, shape, split, least, largest):
    loudness, own = 1.0, jax.random.fold_in(rng, 6)
    for position, blocks in split:
        draws = jnp.exp(jax.random.uniform(jax.random.fold_in(own, position), (blocks,), jnp.float32, least / len(split), largest / len(split)))
        loudness = loudness * jnp.repeat(draws, shape[position] // blocks).reshape([-1 if axis == position else 1 for axis in range(len(shape))])
    return loudness


def cumulative_ranks(number_of, lean):
    portions = [(1 << 20) // math.isqrt(standing ** lean) + 1 for standing in range(1, number_of + 1)]
    deviation = 1 + sum(portions) // (1 << 30)
    return np.cumsum(np.array([max(1, weight // deviation) for weight in portions]))


def ranked(own_key, extent, amount, lean):
    table = cumulative_ranks(amount, lean)
    lot = jax.random.randint(jax.random.fold_in(own_key, 1), extent, 0, int(table[amount - 1]))
    rank = jnp.searchsorted(jnp.asarray(table, jnp.int32), lot, side="right")
    return jax.random.permutation(jax.random.fold_in(own_key, 2), amount)[rank].astype(jnp.int32)


def profile(count, total, reach, skew):
    portions = [(1 << 20) // math.isqrt(grade ** skew) + 1 for grade in range(2, count + 1)]
    surplus, counts = total - reach - (count - 1), [1] * (count - 1)
    while surplus > 0:
        candidates = [i for i in range(count - 1) if counts[i] < reach]
        whole, budget = sum([portions[i] for i in candidates]), surplus
        for i in candidates:
            extra = min(reach - counts[i], max(1, budget * portions[i] // whole), surplus)
            counts[i] = counts[i] + extra
            surplus = surplus - extra
    return np.array([reach] + counts)


def ragged_sizes(rng, number_of, total, bound, skew):
    if number_of == 2:
        one = jax.random.randint(rng, (), max(1, total - bound), min(bound, total - 1) + 1)
        return jnp.stack([one, total - one])
    sizes = jnp.asarray(profile(number_of, total, bound, skew), jnp.int32)
    couples = (number_of - 1) // 2
    giver, sink = sizes[1:1 + 2 * couples:2], sizes[2:2 + 2 * couples:2]
    slack = jnp.minimum(giver - 1, bound - sink)
    moved = jax.random.randint(jax.random.fold_in(rng, 1), (couples,), 0, 1 << 20) % (slack + 1)
    sizes = sizes.at[1:1 + 2 * couples:2].set(giver - moved).at[2:2 + 2 * couples:2].set(sink + moved)
    return sizes[jax.random.permutation(jax.random.fold_in(rng, 2), number_of)]


def centred(key, extent, scale, most, split=(), kind=jnp.bfloat16):
    loudness = shard_levels(key, extent, split, -0.22, 0.18) if split else 1.0
    entries = jax.random.normal(key, extent, jnp.float32) * scale * loudness
    return jnp.minimum(jnp.maximum(entries, -most), most).astype(kind)


def setup_inputs(seed: int = 0) -> dict:
    splits = jax.random.split(jax.random.key(seed), 14)
    return {
        "hidden_in": draw_hidden_in(jax.random.fold_in(splits[13], 71), 0),
        "attn_gain": jnp.clip(1.0 + 0.18 * jax.random.normal(splits[1], (D,), jnp.float32), 0.1, 1.9),
        "w_query": draw_w_query(jax.random.fold_in(splits[13], 71), 0),
        "w_key": draw_w_key(jax.random.fold_in(splits[13], 71), 0),
        "w_value": centred(splits[4], (D, KV_HEADS * HEAD_DIM), D ** -0.5, 0.09375, ((1, 8),)),
        "w_out": centred(splits[5], (HEADS * HEAD_DIM, D), HEAD_DIM ** -0.5, 0.5, ((0, 8),)),
        "final_gain": jnp.clip(1.0 + 0.1 * jax.random.normal(splits[6], (D,), jnp.float32), 0.5, 1.5),
        "teacher_head": draw_teacher_head(jax.random.fold_in(splits[13], 71), 0),
        "draft_rows": centred(splits[8], (TOKENS, DD), 0.25, 1.5, ((0, 16),)),
        "draft_head": draw_draft_head(jax.random.fold_in(splits[13], 71), 0),
        "target_ids": set_ends(ranked(splits[10], (TOKENS,), VOCAB, 2), jax.random.fold_in(splits[10], 3), 0, VOCAB - 1).astype(jnp.int32),
        "rollout_lengths": ragged_sizes(splits[11], ROLLOUTS, TOKENS, TOKENS // 2, 2).astype(jnp.int32),
        "stretch_order": draw_stretch_order(jax.random.fold_in(splits[13], 71), 0),
    }


EPSILON = 1e-05
ROPE_BASE = 500000.0
MIXING = 0.5
NEGATIVE = -1e+30

def rms_scale(values, gain):
    mean_square = lax.optimization_barrier(jnp.mean(values * values, axis=-1, keepdims=True))
    return values * lax.rsqrt(mean_square + EPSILON) * gain

def rotate(vectors, positions):
    half_dim = vectors.shape[-1] // 2
    exponents = jnp.arange(half_dim, dtype=jnp.float32) * (2.0 / vectors.shape[-1])
    frequencies = jnp.power(ROPE_BASE, -exponents)
    angles = positions.astype(jnp.float32)[:, None] * frequencies[None, :]
    cosine_values = jnp.cos(angles)[:, None, :]
    sine_values = jnp.sin(angles)[:, None, :]
    leading = vectors[..., :half_dim]
    trailing = vectors[..., half_dim:]
    return jnp.concatenate([leading * cosine_values - trailing * sine_values, trailing * cosine_values + leading * sine_values], axis=-1)

def slab_positions(stretch_order, rollout_lengths):
    half_rows = TOK_DEV // 2
    row_ids = jnp.arange(TOKENS, dtype=jnp.int32)
    positions = (stretch_order[row_ids // half_rows] * half_rows + row_ids % half_rows).astype(jnp.int32)
    rollout_ends = jnp.cumsum(rollout_lengths).astype(jnp.int32)
    rollouts = lax.optimization_barrier(jnp.sum((positions[:, None] >= rollout_ends[None, :]).astype(jnp.int32), axis=1))
    return (positions, rollouts)

def softmax_rows(logits):
    highest = lax.optimization_barrier(jnp.max(logits, axis=1, keepdims=True))
    weights = jnp.exp(logits - highest)
    return weights / lax.optimization_barrier(jnp.sum(weights, axis=1, keepdims=True))

def row_gradients(final_rows, draft_block, target_block, teacher_head, draft_head):
    word_ids = jnp.arange(VOCAB, dtype=jnp.int32)
    teacher_logits = jnp.dot(final_rows, teacher_head.T, preferred_element_type=jnp.float32)
    draft_logits = jnp.dot(draft_block, draft_head.T, preferred_element_type=jnp.float32)
    teacher_probs = softmax_rows(teacher_logits)
    draft_probs = softmax_rows(draft_logits)
    soft = (1.0 - MIXING) * teacher_probs + jnp.where(target_block[:, None] == word_ids[None, :], MIXING, 0.0)
    delta = (draft_probs - soft).astype(jnp.bfloat16)
    return jnp.dot(delta, draft_head, preferred_element_type=jnp.float32)

def reference(hidden_in, attn_gain, w_query, w_key, w_value, w_out, final_gain, teacher_head, draft_rows, draft_head, target_ids, rollout_lengths, stretch_order):
    group_size = HEADS // KV_HEADS
    positions, rollouts = slab_positions(stretch_order, rollout_lengths)
    normed = rms_scale(hidden_in.astype(jnp.float32), attn_gain).astype(jnp.bfloat16)
    queries = jnp.dot(normed, w_query, preferred_element_type=jnp.float32).reshape(TOKENS, HEADS, HEAD_DIM)
    keys = jnp.dot(normed, w_key, preferred_element_type=jnp.float32).reshape(TOKENS, KV_HEADS, HEAD_DIM)
    values = jnp.dot(normed, w_value, preferred_element_type=jnp.float32).astype(jnp.bfloat16).reshape(TOKENS, KV_HEADS, HEAD_DIM)
    queries = rotate(queries, positions).astype(jnp.bfloat16).reshape(TOKENS, KV_HEADS, group_size, HEAD_DIM)
    keys = rotate(keys, positions).astype(jnp.bfloat16)
    allowed = (positions[None, :] <= positions[:, None]) & (rollouts[None, :] == rollouts[:, None])
    scores = jnp.einsum('qkgd,tkd->kgqt', queries.astype(jnp.float32), keys.astype(jnp.float32)) * HEAD_DIM ** (-0.5)
    scores = jnp.where(allowed[None, None], scores, NEGATIVE)
    highest = lax.optimization_barrier(jnp.max(scores, axis=-1, keepdims=True))
    expd = jnp.where(allowed[None, None], jnp.exp(scores - highest), 0.0)
    totals = lax.optimization_barrier(jnp.sum(expd, axis=-1))
    rounded = lax.optimization_barrier(expd.astype(jnp.bfloat16))
    numerators = jnp.einsum('kgqt,tkd->qkgd', rounded.astype(jnp.float32), values.astype(jnp.float32))
    attended = (numerators / jnp.transpose(totals, (2, 0, 1))[..., None]).astype(jnp.bfloat16).reshape(TOKENS, HEADS * HEAD_DIM)
    mixed = hidden_in.astype(jnp.float32) + jnp.dot(attended, w_out, preferred_element_type=jnp.float32)
    final = rms_scale(mixed, final_gain).astype(jnp.bfloat16)
    blocks = (final.reshape(N_CTX, TOK_DEV, D), draft_rows.reshape(N_CTX, TOK_DEV, DD), target_ids.reshape(N_CTX, TOK_DEV))
    grads = lax.map(lambda block: row_gradients(block[0], block[1], block[2], teacher_head, draft_head), blocks)
    return grads.reshape(TOKENS, DD)
```

```python
import jax
import jax.numpy as jnp
from jax import lax
from jax.experimental import pallas as pl
from jax.experimental.pallas import tpu as pltpu
from jax.sharding import Mesh
from jax.sharding import PartitionSpec as P

HEAD_DIM = 128
EPSILON = 1e-05
ROPE_BASE = 500000.0
MIXING = 0.5
NEGATIVE = -1e30

CTX = ("yh", "z", "c")
VOCAB = ("x", "yl")
X, Y, Z, C = ("x",), ("yh", "yl"), ("z",), ("c",)
CHIPS = ("yh", "z", "x", "yl")
F32, BF16 = jnp.float32, jnp.bfloat16


def shifted(a, axes, k):
    n = lax.axis_size(axes)
    return lax.ppermute(a, axes, [(i, (i + k) % n) for i in range(n)])


def ring(a, axes):
    n = lax.axis_size(axes)
    return [a] + [shifted(a, axes, n - d) for d in range(1, n)]


def rms_scale(values, gain):
    mean_square = jnp.mean(values * values, axis=-1, keepdims=True)
    return values * lax.rsqrt(mean_square + EPSILON) * gain


def rotate(vectors, positions):
    half_dim = vectors.shape[-1] // 2
    exponents = jnp.arange(half_dim, dtype=F32) * (2.0 / vectors.shape[-1])
    frequencies = jnp.power(ROPE_BASE, -exponents)
    angles = positions.astype(F32)[:, None] * frequencies[None, :]
    cosine_values = jnp.cos(angles)[:, None, :]
    sine_values = jnp.sin(angles)[:, None, :]
    leading = vectors[..., :half_dim]
    trailing = vectors[..., half_dim:]
    return jnp.concatenate(
        [
            leading * cosine_values - trailing * sine_values,
            trailing * cosine_values + leading * sine_values,
        ],
        axis=-1,
    )


NT = (((1,), (1,)), ((), ()))


def logits_step(x_ref, head_ref, out_ref, top_ref, sum_ref):
    j = pl.program_id(0)

    @pl.when(j == 0)
    def _():
        top_ref[...] = jnp.full_like(top_ref, NEGATIVE)
        sum_ref[...] = jnp.zeros_like(sum_ref)

    rows = 512

    @pl.loop(0, x_ref.shape[0] // rows)
    def _(i):
        at = pl.ds(pl.multiple_of(i * rows, rows), rows)
        part = lax.dot_general(x_ref[at, :], head_ref[...], NT, preferred_element_type=F32)
        out_ref[at, :] = part
        old = top_ref[at, :]
        new = jnp.maximum(old, jnp.max(part, axis=1, keepdims=True))
        fresh = jnp.sum(jnp.exp(part - new[:, :1]), axis=1, keepdims=True)
        sum_ref[at, :] = sum_ref[at, :] * jnp.exp(old - new) + fresh
        top_ref[at, :] = new


def totals_rows(top_ref, sum_ref):
    lane = lax.broadcasted_iota(jnp.int32, top_ref.shape, 1)
    return jnp.transpose(jnp.where(lane == 0, top_ref[...], sum_ref[...]))


def draft_kernel(rows_ref, head_ref, out_ref, stats_ref, x_ref, top_ref, sum_ref):
    @pl.when(pl.program_id(0) == 0)
    def _():
        for x in range(4):
            for t in range(8):
                x_ref[pl.ds(x * 256 + t * 32, 32), :] = rows_ref[t, x]

    logits_step(x_ref, head_ref, out_ref, top_ref, sum_ref)

    @pl.when(pl.program_id(0) == pl.num_programs(0) - 1)
    def _():
        stats_ref[...] = totals_rows(top_ref, sum_ref)[:8]


def draft_logits(rows, heads):
    words, width = heads.shape
    count = 1024
    block = 256
    return pl.pallas_call(
        draft_kernel,
        grid=(words // block,),
        in_specs=[
            pl.BlockSpec((8, 4, 32, width), lambda j: (0, 0, 0, 0), pipeline_mode=pl.Buffered(1)),
            pl.BlockSpec((block, width), lambda j: (j, 0)),
        ],
        out_specs=[
            pl.BlockSpec((count, block), lambda j: (0, j)),
            pl.BlockSpec((8, count), lambda j: (0, 0)),
        ],
        out_shape=[
            jax.ShapeDtypeStruct((count, words), F32),
            jax.ShapeDtypeStruct((8, count), F32),
        ],
        scratch_shapes=[
            pltpu.VMEM((count, width), BF16),
            pltpu.VMEM((count, 128), F32),
            pltpu.VMEM((count, 128), F32),
        ],
        compiler_params=pltpu.CompilerParams(vmem_limit_bytes=56 << 20),
        cost_estimate=pl.CostEstimate(
            flops=2 * count * words * width, transcendentals=count * words, bytes_accessed=12 << 20
        ),
        name="draft_logits",
    )(rows.reshape(8, 4, 32, width), heads)


def teacher_kernel(place, *refs):
    a_refs, b_refs, c_refs = refs[0:4], refs[4:8], refs[8:12]
    head_ref, draft_stats, out_ref, stats_ref, x_ref, top_ref, sum_ref = refs[12:]

    @pl.when(pl.program_id(0) == 0)
    def _():
        a_width, b_width = a_refs[0].shape[-1], b_refs[0].shape[-1]
        for dx in range(4):
            px = (place[0] + dx) % 4
            for dy in range(4):
                py = (place[1] + dy) % 4
                for dz in range(4):
                    pz = (place[2] + dz) % 4
                    row = px * 256 + (py // 2) * 128 + pz * 32 + (py % 2) * 16
                    at = pl.ds(pl.multiple_of(row, 16), 16)
                    x_ref[at, :a_width] = a_refs[dx][dy, dz]
                    x_ref[at, a_width : a_width + b_width] = b_refs[dy][dx, dz]
                    x_ref[at, a_width + b_width :] = c_refs[dz][dx, dy]

    logits_step(x_ref, head_ref, out_ref, top_ref, sum_ref)

    @pl.when(pl.program_id(0) == pl.num_programs(0) - 1)
    def _():
        rows = totals_rows(top_ref, sum_ref)
        pick = lax.broadcasted_iota(jnp.int32, stats_ref.shape, 0)
        teacher = rows[:8]
        draft = draft_stats[...]
        stats_ref[...] = jnp.where(
            pick == 0,
            teacher[0:1],
            jnp.where(pick == 1, teacher[1:2], jnp.where(pick == 2, draft[0:1], draft[1:2])),
        )


def teacher_logits(place, parts, heads, draft_stats):
    words, width = heads.shape
    count = 1024
    block = 256
    whole = [
        pl.BlockSpec(p.shape, lambda j, s: (0, 0, 0, 0), pipeline_mode=pl.Buffered(1))
        for p in parts
    ]
    return pl.pallas_call(
        teacher_kernel,
        grid_spec=pltpu.PrefetchScalarGridSpec(
            num_scalar_prefetch=1,
            grid=(words // block,),
            in_specs=whole
            + [
                pl.BlockSpec((block, width), lambda j, s: (j, 0)),
                pl.BlockSpec((8, count), lambda j, s: (0, 0)),
            ],
            out_specs=[
                pl.BlockSpec((count, block), lambda j, s: (0, j)),
                pl.BlockSpec((8, count), lambda j, s: (0, 0)),
            ],
            scratch_shapes=[
                pltpu.VMEM((count, width), BF16),
                pltpu.VMEM((count, 128), F32),
                pltpu.VMEM((count, 128), F32),
            ],
        ),
        out_shape=[
            jax.ShapeDtypeStruct((count, words), F32),
            jax.ShapeDtypeStruct((8, count), F32),
        ],
        compiler_params=pltpu.CompilerParams(vmem_limit_bytes=56 << 20),
        cost_estimate=pl.CostEstimate(
            flops=2 * count * words * width, transcendentals=count * words, bytes_accessed=20 << 20
        ),
        name="teacher_logits",
    )(place, *parts, heads, draft_stats)


def gradient_kernel(starts, teacher_ref, draft_ref, rows_ref, head_ref, out_ref, delta_ref):
    count, words = teacher_ref.shape
    column = jnp.transpose(jnp.concatenate([rows_ref[...]] * 16, axis=0))
    half = words // 2
    lane = lax.broadcasted_iota(jnp.int32, (count, half), 1)
    wanted = column[:, 4:5].astype(jnp.int32)
    for h in range(2):
        at = slice(h * half, (h + 1) * half)
        teacher = jnp.exp(teacher_ref[:, at] - column[:, 0:1]) * column[:, 1:2]
        draft = jnp.exp(draft_ref[:, at] - column[:, 2:3]) * column[:, 3:4]
        soft = teacher + jnp.where(lane + starts[h] == wanted, MIXING, 0.0)
        delta_ref[:, at] = (draft - soft).astype(BF16)

    @pl.loop(0, 8)
    def _(f):
        at = pl.ds(pl.multiple_of(f * 256, 256), 256)
        part = jnp.dot(delta_ref[...], head_ref[:, at], preferred_element_type=F32).astype(BF16)
        for x in range(count // 256):
            for t in range(8):
                out_ref[t, f, x] = part[x * 256 + t * 32 : x * 256 + t * 32 + 32]


def gradient_parts(starts, teacher, draft, rows, heads):
    count, words = teacher.shape
    width = heads.shape[1]
    tile = 512
    return pl.pallas_call(
        gradient_kernel,
        grid_spec=pltpu.PrefetchScalarGridSpec(
            num_scalar_prefetch=1,
            grid=(count // tile,),
            in_specs=[
                pl.BlockSpec((tile, words), lambda j, s: (j, 0)),
                pl.BlockSpec((tile, words), lambda j, s: (j, 0)),
                pl.BlockSpec((8, tile), lambda j, s: (0, j)),
                pl.BlockSpec((words, width), lambda j, s: (0, 0), pipeline_mode=pl.Buffered(1)),
            ],
            out_specs=pl.BlockSpec((8, 8, tile // 256, 32, 256), lambda j, s: (0, 0, j, 0, 0)),
            scratch_shapes=[pltpu.VMEM((tile, words), BF16)],
        ),
        out_shape=jax.ShapeDtypeStruct((8, 8, 4, 32, 256), BF16),
        compiler_params=pltpu.CompilerParams(vmem_limit_bytes=56 << 20),
        cost_estimate=pl.CostEstimate(
            flops=2 * count * words * width, transcendentals=2 * count * words, bytes_accessed=16 << 20
        ),
        name="gradient_parts",
    )(starts, teacher, draft, rows, heads)


def merge_totals(pieces):
    tops = [(p[0], p[2]) for p in pieces]
    sums = [(p[1], p[3]) for p in pieces]
    out = []
    for k in range(2):
        top = tops[0][k]
        for other in tops[1:]:
            top = jnp.maximum(top, other[k])
        total = sum(s[k] * jnp.exp(t[k] - top) for t, s in zip(tops, sums))
        out += [top, total]
    return jnp.stack(out)


def on_device(
    hidden_in,
    attn_gain,
    w_query,
    w_key,
    w_value,
    w_out,
    final_gain,
    teacher_head,
    draft_rows,
    draft_head,
    target_ids,
    rollout_lengths,
    stretch_order,
):
    row_count = hidden_in.shape[0]
    head_dim = HEAD_DIM
    local_heads = w_query.shape[1] // head_dim
    local_groups = w_key.shape[1] // head_dim
    group_size = local_heads // local_groups
    half_rows = row_count // 2
    stretch_ids = jnp.arange(stretch_order.shape[0], dtype=jnp.int32)
    rollout_ends = jnp.cumsum(rollout_lengths)
    my_x, my_yh, my_yl = lax.axis_index("x"), lax.axis_index("yh"), lax.axis_index("yl")
    my_z, my_c = lax.axis_index("z"), lax.axis_index("c")

    def locate(row_ids):
        stretch_hit = (row_ids // half_rows)[:, None] == stretch_ids[None, :]
        stretch_start = jnp.sum(jnp.where(stretch_hit, stretch_order[None, :], 0), axis=1)
        positions = stretch_start * half_rows + row_ids % half_rows
        rollouts = jnp.sum((positions[:, None] >= rollout_ends[None, :]).astype(jnp.int32), axis=1)
        return (positions, rollouts)

    lines = jnp.arange(row_count, dtype=jnp.int32)
    query_pos, query_roll = locate(lax.axis_index(CTX) * row_count + lines)
    normed = rms_scale(hidden_in.astype(F32), attn_gain).astype(BF16)
    keys = jnp.dot(normed, w_key, preferred_element_type=F32).reshape(
        row_count, local_groups, head_dim
    )
    keys = rotate(keys, query_pos).astype(BF16).reshape(row_count, local_groups * head_dim)
    values = jnp.dot(normed, w_value, preferred_element_type=F32).astype(BF16)
    both = jnp.concatenate([keys, values], axis=1)
    both = jnp.concatenate(ring(both, ("yh",)), axis=0)
    both = jnp.concatenate(ring(both, Z), axis=0)
    both = jnp.concatenate(ring(both, C), axis=0)
    key_width = local_groups * head_dim
    key_piece = both[:, :key_width].reshape(-1, local_groups, head_dim)
    value_piece = both[:, key_width:].reshape(-1, local_groups, head_dim)

    queries = jnp.dot(normed, w_query, preferred_element_type=F32).reshape(
        row_count, local_heads, head_dim
    )
    queries = (
        rotate(queries, query_pos)
        .astype(BF16)
        .reshape(row_count, local_groups, group_size, head_dim)
    )
    slots = jnp.arange(key_piece.shape[0], dtype=jnp.int32)
    slot = slots // row_count
    from_c = (my_c + slot // 8) % 2
    from_z = (my_z + (slot // 2) % 4) % 4
    from_yh = (my_yh + slot % 2) % 2
    owner = (from_yh * 4 + from_z) * 2 + from_c
    key_pos, key_roll = locate(owner * row_count + slots % row_count)
    allowed = (key_pos[None, :] <= query_pos[:, None]) & (key_roll[None, :] == query_roll[:, None])
    visible = allowed[:, None, None, :]
    scores = jnp.einsum(
        "tkgd,nkd->tkgn", queries, key_piece, preferred_element_type=F32
    ) * head_dim ** (-0.5)
    scores = jnp.where(visible, scores, NEGATIVE)
    top = jnp.max(scores, axis=-1)
    weights = jnp.where(visible, jnp.exp(scores - top[..., None]), 0.0)
    weight_sum = jnp.sum(weights, axis=-1)
    weighted = jnp.einsum(
        "tkgn,nkd->tkgd", weights.astype(BF16), value_piece, preferred_element_type=F32
    )
    attended = (
        (weighted / weight_sum[..., None]).astype(BF16).reshape(row_count, local_heads * head_dim)
    )

    partial_value = jnp.dot(attended, w_out, preferred_element_type=F32).astype(BF16)
    shares = lax.axis_size(VOCAB)
    share_rows = row_count // shares
    arrived = lax.all_to_all(
        partial_value.reshape(shares, share_rows, -1), VOCAB, split_axis=0, concat_axis=0, tiled=True
    )
    own_rows = lax.dynamic_slice_in_dim(
        hidden_in, lax.axis_index(VOCAB) * share_rows, share_rows, 0
    )
    mixed = own_rows.astype(F32) + jnp.sum(arrived.astype(F32), axis=0)
    final = rms_scale(mixed, final_gain).astype(BF16)

    teacher_heads = jnp.concatenate([teacher_head, shifted(teacher_head, C, 1)], axis=0)
    draft_heads = jnp.concatenate([draft_head, shifted(draft_head, C, 1)], axis=0)

    draft_all = lax.all_gather(draft_rows, ("yh", "z"), axis=0, tiled=True)
    draft_part, draft_stats = draft_logits(draft_all, draft_heads)

    a, b, c = jnp.split(final, [1408, 2816], axis=1)
    a = jnp.stack(ring(a, Z))
    b = jnp.stack(ring(b, X))
    c = jnp.stack(ring(c, Y))
    a = jnp.stack(ring(a, Y))
    b = jnp.stack(ring(b, Z), axis=1)
    c = jnp.stack(ring(c, X))
    a, b, c = ring(a, X), ring(b, Y), ring(c, Z)
    place = jnp.stack([my_x, my_yh * 2 + my_yl, my_z]).astype(jnp.int32)
    teacher_part, stats = teacher_logits(place, a + b + c, teacher_heads, draft_stats)

    for axes in (X, Y, Z):
        stats = merge_totals(ring(stats, axes))
    targets = target_ids.reshape(2, 4, 2, 4, 2 * share_rows)
    targets = lax.dynamic_index_in_dim(targets, my_c, 2, keepdims=False)
    targets = jnp.transpose(targets, (2, 0, 1, 3)).reshape(-1).astype(F32)
    nothing = jnp.zeros_like(targets)
    rows = jnp.stack(
        [
            stats[0],
            (1.0 - MIXING) / stats[1],
            stats[2],
            1.0 / stats[3],
            targets,
            nothing,
            nothing,
            nothing,
        ]
    )
    word_count = teacher_head.shape[0]
    block_id = lax.axis_index(VOCAB) * lax.axis_size(CTX) + (my_yh * 4 + my_z) * 2
    starts = jnp.stack([block_id + my_c, block_id + 1 - my_c]).astype(jnp.int32) * word_count
    parts = gradient_parts(starts, teacher_part, draft_part, rows, draft_heads)
    parts = parts.reshape(64, row_count, -1)
    arrived = lax.all_to_all(parts, CHIPS, split_axis=0, concat_axis=0, tiled=True)
    return jnp.sum(arrived.astype(F32), axis=0)


def solution(mesh):
    torus = Mesh(mesh.devices.reshape(2, 4, 2, 4, 2), ("yh", "z", "c", "x", "yl"))
    words = P(("x", "yl", "yh", "z", "c"), None)
    return jax.shard_map(
        on_device,
        mesh=torus,
        in_specs=(
            P(CTX, None),
            P(),
            P(None, VOCAB),
            P(None, VOCAB),
            P(None, VOCAB),
            P(VOCAB, None),
            P(),
            words,
            P(CTX, None),
            words,
            P(),
            P(),
            P(),
        ),
        out_specs=P(CTX, VOCAB),
        check_vma=False,
    )
```

```python
import jax
import jax.numpy as jnp
from jax import lax
from jax.experimental import pallas as pl
from jax.experimental.pallas import tpu as pltpu
from jax.sharding import Mesh
from jax.sharding import PartitionSpec as P


HEAD_DIM = 128
EPSILON = 1e-05
ROPE_BASE = 500000.0
MIXING = 0.5
NEGATIVE = -1e30

CTX = ("yh", "z", "c")
VOCAB = ("x", "yl")
X, Y, Z, C = ("x",), ("yh", "yl"), ("z",), ("c",)
CHIPS = ("yh", "z", "x", "yl")
F32, BF16 = jnp.float32, jnp.bfloat16


def shifted(a, axes, k):
    n = lax.axis_size(axes)
    return lax.ppermute(a, axes, [(i, (i + k) % n) for i in range(n)])


def ring(a, axes):
    n = lax.axis_size(axes)
    return [a] + [shifted(a, axes, n - d) for d in range(1, n)]


def rms_scale(values, gain):
    mean_square = jnp.mean(values * values, axis=-1, keepdims=True)
    return values * lax.rsqrt(mean_square + EPSILON) * gain


def rotate(vectors, positions):
    half_dim = vectors.shape[-1] // 2
    exponents = jnp.arange(half_dim, dtype=F32) * (2.0 / vectors.shape[-1])
    frequencies = jnp.power(ROPE_BASE, -exponents)
    angles = positions.astype(F32)[:, None] * frequencies[None, :]
    cosine_values = jnp.cos(angles)[:, None, :]
    sine_values = jnp.sin(angles)[:, None, :]
    leading = vectors[..., :half_dim]
    trailing = vectors[..., half_dim:]
    return jnp.concatenate(
        [
            leading * cosine_values - trailing * sine_values,
            trailing * cosine_values + leading * sine_values,
        ],
        axis=-1,
    )


NT = (((1,), (1,)), ((), ()))


BLOCK = 256


def fetch_words(own_ref, other_ref, held_ref, arrived):
    j, steps = pl.program_id(0), pl.num_programs(0)
    half = steps // 2

    def start(step, slot):
        @pl.when(step < half)
        def _():
            at = pl.ds(pl.multiple_of(step * BLOCK, BLOCK), BLOCK)
            pltpu.make_async_copy(own_ref.at[at], held_ref.at[slot], arrived.at[slot]).start()

        @pl.when(step >= half)
        def _():
            at = pl.ds(pl.multiple_of((step - half) * BLOCK, BLOCK), BLOCK)
            pltpu.make_async_copy(other_ref.at[at], held_ref.at[slot], arrived.at[slot]).start()

    @pl.when(j == 0)
    def _():
        start(0, 0)

    @pl.when(j + 1 < steps)
    def _():
        start(j + 1, (j + 1) % 2)

    slot = j % 2
    pltpu.make_async_copy(own_ref.at[pl.ds(0, BLOCK)], held_ref.at[slot], arrived.at[slot]).wait()
    return slot


def logits_step(slot, x_ref, held_ref, out_ref, top_ref, sum_ref):
    @pl.when(pl.program_id(0) == 0)
    def _():
        top_ref[...] = jnp.full_like(top_ref, NEGATIVE)
        sum_ref[...] = jnp.zeros_like(sum_ref)

    part = lax.dot_general(x_ref[...], held_ref[slot], NT, preferred_element_type=F32)
    out_ref[...] = part
    pieces = [part[:, k : k + 128] for k in range(0, BLOCK, 128)]
    old = top_ref[...]
    new = old
    for piece in pieces:
        new = jnp.maximum(new, piece)
    total = sum_ref[...] * jnp.exp(old - new)
    for piece in pieces:
        total = total + jnp.exp(piece - new)
    sum_ref[...] = total
    top_ref[...] = new


def totals_rows(top_ref, sum_ref):
    shape = top_ref.shape
    lanes = top_ref[...]
    top = jnp.max(lanes, axis=1, keepdims=True)
    total = jnp.sum(sum_ref[...] * jnp.exp(lanes - top), axis=1, keepdims=True)
    lane = lax.broadcasted_iota(jnp.int32, shape, 1)
    both = jnp.where(lane == 0, jnp.broadcast_to(top, shape), jnp.broadcast_to(total, shape))
    return jnp.transpose(both)


HELD = pl.BlockSpec(memory_space=pltpu.HBM)


def logits_scratch(count, width):
    return [
        pltpu.VMEM((count, width), BF16),
        pltpu.VMEM((2, BLOCK, width), BF16),
        pltpu.SemaphoreType.DMA((2,)),
        pltpu.VMEM((count, 128), F32),
        pltpu.VMEM((count, 128), F32),
    ]


def draft_kernel(place, *refs):
    near_ref, ahead_ref, behind_ref = refs[0:3]
    own_ref, other_ref, out_ref, stats_ref, x_ref, held_ref, arrived, top_ref, sum_ref = refs[5:]
    slot = fetch_words(own_ref, other_ref, held_ref, arrived)

    @pl.when(pl.program_id(0) == 0)
    def _():
        for dz in range(4):
            pz = (place[2] + dz) % 4
            for dyh in range(2):
                base = (place[1] // 2 + dyh) % 2 * 128 + pz * 32
                for x in range(4):
                    at = pl.ds(pl.multiple_of(base + x * 256, 32), 32)
                    if dz == 2:
                        x_ref[at, :] = refs[3 + dyh][x]
                    else:
                        x_ref[at, :] = (near_ref, ahead_ref, None, behind_ref)[dz][dyh, x]

    logits_step(slot, x_ref, held_ref, out_ref, top_ref, sum_ref)

    @pl.when(pl.program_id(0) == pl.num_programs(0) - 1)
    def _():
        stats_ref[...] = totals_rows(top_ref, sum_ref)[:8]


def draft_logits(place, rows, own, other):
    words, width = 2 * own.shape[0], own.shape[1]
    count = 1024
    return pl.pallas_call(
        draft_kernel,
        grid_spec=pltpu.PrefetchScalarGridSpec(
            num_scalar_prefetch=1,
            grid=(words // BLOCK,),
            in_specs=[
                pl.BlockSpec(r.shape, lambda j, s, n=r.ndim: (0,) * n, pipeline_mode=pl.Buffered(1))
                for r in rows
            ]
            + [HELD, HELD],
            out_specs=[
                pl.BlockSpec((count, BLOCK), lambda j, s: (0, j)),
                pl.BlockSpec((8, count), lambda j, s: (0, 0)),
            ],
            scratch_shapes=logits_scratch(count, width),
        ),
        out_shape=[
            jax.ShapeDtypeStruct((count, words), F32),
            jax.ShapeDtypeStruct((8, count), F32),
        ],
        compiler_params=pltpu.CompilerParams(vmem_limit_bytes=40 << 20),
        cost_estimate=pl.CostEstimate(
            flops=2 * count * words * width, transcendentals=count * words, bytes_accessed=12 << 20
        ),
        name="draft_logits",
    )(place, *rows, own, other)


def teacher_kernel(place, *refs):
    a_refs, b_refs, c_refs = refs[0:4], refs[4:8], refs[8:12]
    own_ref, other_ref, draft_stats, out_ref, stats_ref = refs[12:17]
    x_ref, held_ref, arrived, top_ref, sum_ref = refs[17:]
    slot = fetch_words(own_ref, other_ref, held_ref, arrived)

    @pl.when(pl.program_id(0) == 0)
    def _():
        a_width, b_width = a_refs[0].shape[-1], b_refs[0].shape[-1]
        for dx in range(4):
            px = (place[0] + dx) % 4
            for dy in range(4):
                py = (place[1] + dy) % 4
                for dz in range(4):
                    pz = (place[2] + dz) % 4
                    row = px * 256 + (py // 2) * 128 + pz * 32 + (py % 2) * 16
                    at = pl.ds(pl.multiple_of(row, 16), 16)
                    x_ref[at, :a_width] = a_refs[dx][dy, dz]
                    x_ref[at, a_width : a_width + b_width] = b_refs[dy][dz, dx]
                    x_ref[at, a_width + b_width :] = c_refs[dz][dx, dy]

    logits_step(slot, x_ref, held_ref, out_ref, top_ref, sum_ref)

    @pl.when(pl.program_id(0) == pl.num_programs(0) - 1)
    def _():
        teacher = totals_rows(top_ref, sum_ref)
        stats_ref[...] = jnp.concatenate([teacher[0:2], draft_stats[0:2], teacher[4:8]], axis=0)


def teacher_logits(place, parts, own, other, draft_stats):
    words, width = 2 * own.shape[0], own.shape[1]
    count = 1024
    whole = [
        pl.BlockSpec(p.shape, lambda j, s: (0, 0, 0, 0), pipeline_mode=pl.Buffered(1))
        for p in parts
    ]
    return pl.pallas_call(
        teacher_kernel,
        grid_spec=pltpu.PrefetchScalarGridSpec(
            num_scalar_prefetch=1,
            grid=(words // BLOCK,),
            in_specs=whole + [HELD, HELD, pl.BlockSpec((8, count), lambda j, s: (0, 0))],
            out_specs=[
                pl.BlockSpec((count, BLOCK), lambda j, s: (0, j)),
                pl.BlockSpec((8, count), lambda j, s: (0, 0)),
            ],
            scratch_shapes=logits_scratch(count, width),
        ),
        out_shape=[
            jax.ShapeDtypeStruct((count, words), F32),
            jax.ShapeDtypeStruct((8, count), F32),
        ],
        compiler_params=pltpu.CompilerParams(vmem_limit_bytes=48 << 20),
        cost_estimate=pl.CostEstimate(
            flops=2 * count * words * width, transcendentals=count * words, bytes_accessed=20 << 20
        ),
        name="teacher_logits",
    )(place, *parts, own, other, draft_stats)


def gradient_kernel(starts, teacher_ref, draft_ref, rows_ref, own_ref, other_ref, out_ref, delta_ref):
    count, words = teacher_ref.shape
    column = jnp.transpose(jnp.concatenate([rows_ref[...]] * 16, axis=0))
    half = words // 2
    lane = lax.broadcasted_iota(jnp.int32, (count, half), 1)
    wanted = column[:, 4:5].astype(jnp.int32)
    for h in range(2):
        at = slice(h * half, (h + 1) * half)
        teacher = jnp.exp(teacher_ref[:, at] - column[:, 0:1]) * column[:, 1:2]
        draft = jnp.exp(draft_ref[:, at] - column[:, 2:3]) * column[:, 3:4]
        soft = teacher + jnp.where(lane + starts[h] == wanted, MIXING, 0.0)
        delta_ref[:, at] = (draft - soft).astype(BF16)
    total = jnp.dot(delta_ref[:, :half], own_ref[...], preferred_element_type=F32)
    total = total + jnp.dot(delta_ref[:, half:], other_ref[...], preferred_element_type=F32)
    total = total.astype(BF16)
    for f in range(8):
        for t in range(8):
            out_ref[t, f, 0] = total[t * 32 : t * 32 + 32, f * 256 : f * 256 + 256]


def gradient_parts(starts, teacher, draft, rows, own, other):
    count, words = teacher.shape
    width = own.shape[1]
    tile = 256
    held = pl.BlockSpec(own.shape, lambda j, s: (0, 0), pipeline_mode=pl.Buffered(1))
    return pl.pallas_call(
        gradient_kernel,
        grid_spec=pltpu.PrefetchScalarGridSpec(
            num_scalar_prefetch=1,
            grid=(count // tile,),
            in_specs=[
                pl.BlockSpec((tile, words), lambda j, s: (j, 0)),
                pl.BlockSpec((tile, words), lambda j, s: (j, 0)),
                pl.BlockSpec((8, tile), lambda j, s: (0, j)),
                held,
                held,
            ],
            out_specs=pl.BlockSpec((8, 8, 1, 32, 256), lambda j, s: (0, 0, j, 0, 0)),
            scratch_shapes=[pltpu.VMEM((tile, words), BF16)],
        ),
        out_shape=jax.ShapeDtypeStruct((8, 8, 4, 32, 256), BF16),
        compiler_params=pltpu.CompilerParams(vmem_limit_bytes=40 << 20),
        cost_estimate=pl.CostEstimate(
            flops=2 * count * words * width, transcendentals=2 * count * words, bytes_accessed=16 << 20
        ),
        name="gradient_parts",
    )(starts, teacher, draft, rows, own, other)


def on_device(
    hidden_in,
    attn_gain,
    w_query,
    w_key,
    w_value,
    w_out,
    final_gain,
    teacher_head,
    draft_rows,
    draft_head,
    target_ids,
    rollout_lengths,
    stretch_order,
):
    row_count = hidden_in.shape[0]
    head_dim = HEAD_DIM
    local_heads = w_query.shape[1] // head_dim
    local_groups = w_key.shape[1] // head_dim
    group_size = local_heads // local_groups
    half_rows = row_count // 2
    stretch_ids = jnp.arange(stretch_order.shape[0], dtype=jnp.int32)
    rollout_ends = jnp.cumsum(rollout_lengths)
    my_x, my_yh, my_yl = lax.axis_index("x"), lax.axis_index("yh"), lax.axis_index("yl")
    my_z, my_c = lax.axis_index("z"), lax.axis_index("c")

    def locate(row_ids):
        stretch_hit = (row_ids // half_rows)[:, None] == stretch_ids[None, :]
        stretch_start = jnp.sum(jnp.where(stretch_hit, stretch_order[None, :], 0), axis=1)
        positions = stretch_start * half_rows + row_ids % half_rows
        rollouts = jnp.sum((positions[:, None] >= rollout_ends[None, :]).astype(jnp.int32), axis=1)
        return (positions, rollouts)

    lines = jnp.arange(row_count, dtype=jnp.int32)
    query_pos, query_roll = locate(lax.axis_index(CTX) * row_count + lines)
    normed = rms_scale(hidden_in.astype(F32), attn_gain).astype(BF16)
    keys = jnp.dot(normed, w_key, preferred_element_type=F32).reshape(
        row_count, local_groups, head_dim
    )
    keys = rotate(keys, query_pos).astype(BF16).reshape(row_count, local_groups * head_dim)
    values = jnp.dot(normed, w_value, preferred_element_type=F32).astype(BF16)
    both = jnp.concatenate([keys, values], axis=1)
    copies = jnp.broadcast_to(both[None], (8, *both.shape))
    both = lax.all_to_all(copies, ("yh", "z"), split_axis=0, concat_axis=0, tiled=True)
    gathered = both
    both = both.reshape(8 * row_count, -1)
    both = jnp.concatenate(ring(both, C), axis=0)
    key_width = local_groups * head_dim
    key_piece = both[:, :key_width].reshape(-1, local_groups, head_dim)
    value_piece = both[:, key_width:].reshape(-1, local_groups, head_dim)

    queries = jnp.dot(normed, w_query, preferred_element_type=F32).reshape(
        row_count, local_heads, head_dim
    )
    queries = (
        rotate(queries, query_pos)
        .astype(BF16)
        .reshape(row_count, local_groups, group_size, head_dim)
    )
    slots = jnp.arange(key_piece.shape[0], dtype=jnp.int32)
    slot = slots // row_count
    from_c = (my_c + slot // 8) % 2
    owner = slot % 8 * 2 + from_c
    key_pos, key_roll = locate(owner * row_count + slots % row_count)
    allowed = (key_pos[None, :] <= query_pos[:, None]) & (key_roll[None, :] == query_roll[:, None])
    visible = allowed[:, None, None, :]
    scores = jnp.einsum(
        "tkgd,nkd->tkgn", queries, key_piece, preferred_element_type=F32
    ) * head_dim ** (-0.5)
    scores = jnp.where(visible, scores, NEGATIVE)
    top = jnp.max(scores, axis=-1)
    weights = jnp.where(visible, jnp.exp(scores - top[..., None]), 0.0)
    weight_sum = jnp.sum(weights, axis=-1)
    weighted = jnp.einsum(
        "tkgn,nkd->tkgd", weights.astype(BF16), value_piece, preferred_element_type=F32
    )
    attended = (
        (weighted / weight_sum[..., None]).astype(BF16).reshape(row_count, local_heads * head_dim)
    )

    partial_value = jnp.dot(attended, w_out, preferred_element_type=F32).astype(BF16)
    shares = lax.axis_size(VOCAB)
    share_rows = row_count // shares
    arrived = lax.all_to_all(
        partial_value.reshape(shares, share_rows, -1),
        VOCAB,
        split_axis=0,
        concat_axis=0,
        tiled=True,
    )
    own_rows = lax.dynamic_slice_in_dim(
        hidden_in, lax.axis_index(VOCAB) * share_rows, share_rows, 0
    )
    mixed = own_rows.astype(F32) + jnp.sum(arrived.astype(F32), axis=0)
    final = rms_scale(mixed, final_gain).astype(BF16)

    teacher_other = shifted(teacher_head, C, 1)
    draft_other = shifted(draft_head, C, 1)

    place = jnp.stack([my_x, my_yh * 2 + my_yl, my_z]).astype(jnp.int32)
    near = jnp.stack(ring(draft_rows, ("yh",)))
    near, _ = lax.optimization_barrier((near, gathered))
    near = near.reshape(2, 4, 2 * share_rows, -1)
    ahead, behind = shifted(near, Z, 3), shifted(near, Z, 1)
    far = [shifted(ahead[0], Z, 3), shifted(behind[1], Z, 1)]
    draft_part, draft_stats = draft_logits(
        place, [near, ahead, behind] + far, draft_head, draft_other
    )

    a, b, c = jnp.split(final, [1408, 2816], axis=1)
    a, b, c = ring(a, Z), ring(b, X), ring(c, Y)
    a, b, c = jnp.stack(a), jnp.stack(b), jnp.stack(c)
    a = jnp.stack(ring(a, Y))
    b = jnp.stack(ring(b, Z))
    c = jnp.stack(ring(c, X))
    a, b, c = ring(a, X), ring(b, Y), ring(c, Z)
    teacher_part, stats = teacher_logits(
        place, a + b + c, teacher_head, teacher_other, draft_stats
    )

    for axes in (("x", "yl"), ("yh", "z")):
        copies = jnp.broadcast_to(stats[None, :4], (8, *stats[:4].shape))
        pieces = lax.all_to_all(copies, axes, split_axis=0, concat_axis=0, tiled=True)
        tops = jnp.max(pieces[:, 0::2], axis=0)
        sums = jnp.sum(pieces[:, 1::2] * jnp.exp(pieces[:, 0::2] - tops), axis=0)
        stats = jnp.stack([tops[0], sums[0], tops[1], sums[1]])
    targets = target_ids.reshape(2, 4, 2, 4, 2 * share_rows)
    targets = lax.dynamic_index_in_dim(targets, my_c, 2, keepdims=False)
    targets = jnp.transpose(targets, (2, 0, 1, 3)).reshape(-1).astype(F32)
    nothing = jnp.zeros_like(targets)
    rows = jnp.stack(
        [
            stats[0],
            (1.0 - MIXING) / stats[1],
            stats[2],
            1.0 / stats[3],
            targets,
            nothing,
            nothing,
            nothing,
        ]
    )
    word_count = teacher_head.shape[0]
    block_id = lax.axis_index(VOCAB) * lax.axis_size(CTX) + (my_yh * 4 + my_z) * 2
    starts = jnp.stack([block_id + my_c, block_id + 1 - my_c]).astype(jnp.int32) * word_count
    parts = gradient_parts(starts, teacher_part, draft_part, rows, draft_head, draft_other)
    parts = parts.reshape(64, row_count, -1)
    arrived = lax.all_to_all(parts, CHIPS, split_axis=0, concat_axis=0, tiled=True)
    return jnp.sum(arrived.astype(F32), axis=0)


def solution(mesh):
    torus = Mesh(mesh.devices.reshape(2, 4, 2, 4, 2), ("yh", "z", "c", "x", "yl"))
    words = P(("x", "yl", "yh", "z", "c"), None)

    return jax.shard_map(
        on_device,
        mesh=torus,
        in_specs=(
            P(CTX, None),
            P(),
            P(None, VOCAB),
            P(None, VOCAB),
            P(None, VOCAB),
            P(VOCAB, None),
            P(),
            words,
            P(CTX, None),
            words,
            P(),
            P(),
            P(),
        ),
        out_specs=P(CTX, VOCAB),
        check_vma=False,
    )
```

```python
import jax
import jax.numpy as jnp
from jax import lax
from jax.experimental import pallas as pl
from jax.experimental.pallas import tpu as pltpu
from jax.sharding import Mesh
from jax.sharding import PartitionSpec as P


HEAD_DIM = 128
EPSILON = 1e-05
ROPE_BASE = 500000.0
MIXING = 0.5
NEGATIVE = -1e30

CTX = ("yh", "z", "c")
VOCAB = ("x", "yl")
Z, C = ("z",), ("c",)
CHIPS = ("yh", "z", "x", "yl")
F32, BF16 = jnp.float32, jnp.bfloat16


def shifted(a, axes, k):
    n = lax.axis_size(axes)
    return lax.ppermute(a, axes, [(i, (i + k) % n) for i in range(n)])


def ring(a, axes):
    n = lax.axis_size(axes)
    return [a] + [shifted(a, axes, n - d) for d in range(1, n)]


EVERY = ("yh", "z", "c", "x", "yl")


def moved(a, along, k):
    pairs = []
    for source in range(128):
        yh, z, c = source // 64, source // 16 % 4, source // 8 % 2
        x, yl = source // 2 % 4, source % 2
        y = 2 * yh + yl
        x = (x + k) % 4 if along[c] == "x" else x
        y = (y + k) % 4 if along[c] == "y" else y
        z = (z + k) % 4 if along[c] == "z" else z
        pairs.append((source, (((y // 2 * 4 + z) * 2 + c) * 4 + x) * 2 + y % 2))
    return lax.ppermute(a, EVERY, pairs)


def spread(a, along):
    return [a] + [moved(a, along, 4 - d) for d in range(1, 4)]


def rms_scale(values, gain):
    mean_square = jnp.mean(values * values, axis=-1, keepdims=True)
    return values * lax.rsqrt(mean_square + EPSILON) * gain


def rotate(vectors, positions):
    half_dim = vectors.shape[-1] // 2
    exponents = jnp.arange(half_dim, dtype=F32) * (2.0 / vectors.shape[-1])
    frequencies = jnp.power(ROPE_BASE, -exponents)
    angles = positions.astype(F32)[:, None] * frequencies[None, :]
    cosine_values = jnp.cos(angles)[:, None, :]
    sine_values = jnp.sin(angles)[:, None, :]
    leading = vectors[..., :half_dim]
    trailing = vectors[..., half_dim:]
    return jnp.concatenate(
        [
            leading * cosine_values - trailing * sine_values,
            trailing * cosine_values + leading * sine_values,
        ],
        axis=-1,
    )


NT = (((1,), (1,)), ((), ()))


BLOCK = 256


def fetch_words(own_ref, other_ref, held_ref, arrived):
    j, steps = pl.program_id(0), pl.num_programs(0)
    half = steps // 2

    def start(step, slot):
        @pl.when(step < half)
        def _():
            at = pl.ds(pl.multiple_of(step * BLOCK, BLOCK), BLOCK)
            pltpu.make_async_copy(own_ref.at[at], held_ref.at[slot], arrived.at[slot]).start()

        @pl.when(step >= half)
        def _():
            at = pl.ds(pl.multiple_of((step - half) * BLOCK, BLOCK), BLOCK)
            pltpu.make_async_copy(other_ref.at[at], held_ref.at[slot], arrived.at[slot]).start()

    @pl.when(j == 0)
    def _():
        start(0, 0)

    @pl.when(j + 1 < steps)
    def _():
        start(j + 1, (j + 1) % 2)

    slot = j % 2
    pltpu.make_async_copy(own_ref.at[pl.ds(0, BLOCK)], held_ref.at[slot], arrived.at[slot]).wait()
    return slot


def logits_step(slot, x_ref, held_ref, out_ref, top_ref, sum_ref):
    @pl.when(pl.program_id(0) == 0)
    def _():
        top_ref[...] = jnp.full_like(top_ref, NEGATIVE)
        sum_ref[...] = jnp.zeros_like(sum_ref)

    part = lax.dot_general(x_ref[...], held_ref[slot], NT, preferred_element_type=F32)
    out_ref[...] = part
    pieces = [part[:, k : k + 128] for k in range(0, BLOCK, 128)]
    old = top_ref[...]
    new = old
    for piece in pieces:
        new = jnp.maximum(new, piece)
    total = sum_ref[...] * jnp.exp(old - new)
    for piece in pieces:
        total = total + jnp.exp(piece - new)
    sum_ref[...] = total
    top_ref[...] = new


def totals_rows(top_ref, sum_ref):
    shape = top_ref.shape
    lanes = top_ref[...]
    top = jnp.max(lanes, axis=1, keepdims=True)
    total = jnp.sum(sum_ref[...] * jnp.exp(lanes - top), axis=1, keepdims=True)
    lane = lax.broadcasted_iota(jnp.int32, shape, 1)
    both = jnp.where(lane == 0, jnp.broadcast_to(top, shape), jnp.broadcast_to(total, shape))
    return jnp.transpose(both)


HELD = pl.BlockSpec(memory_space=pltpu.HBM)


def logits_scratch(count, width):
    return [
        pltpu.VMEM((count, width), BF16),
        pltpu.VMEM((2, BLOCK, width), BF16),
        pltpu.SemaphoreType.DMA((2,)),
        pltpu.VMEM((count, 128), F32),
        pltpu.VMEM((count, 128), F32),
    ]


def draft_kernel(place, *refs):
    row_refs = refs[0:8]
    own_ref, other_ref, out_ref, stats_ref, x_ref, held_ref, arrived, top_ref, sum_ref = refs[8:]
    slot = fetch_words(own_ref, other_ref, held_ref, arrived)

    @pl.when(pl.program_id(0) == 0)
    def _():
        for dyh in range(2):
            for dz in range(4):
                base = place[12 + dyh] + place[8 + dz]
                for x in range(4):
                    at = pl.ds(pl.multiple_of(base + x * 256, 32), 32)
                    x_ref[at, :] = row_refs[dyh * 4 + dz][x]

    logits_step(slot, x_ref, held_ref, out_ref, top_ref, sum_ref)

    @pl.when(pl.program_id(0) == pl.num_programs(0) - 1)
    def _():
        stats_ref[...] = totals_rows(top_ref, sum_ref)[:8]


def draft_logits(place, rows, own, other):
    words, width = 2 * own.shape[0], own.shape[1]
    count = 1024
    return pl.pallas_call(
        draft_kernel,
        grid_spec=pltpu.PrefetchScalarGridSpec(
            num_scalar_prefetch=1,
            grid=(words // BLOCK,),
            in_specs=[
                pl.BlockSpec(r.shape, lambda j, s, n=r.ndim: (0,) * n, pipeline_mode=pl.Buffered(1))
                for r in rows
            ]
            + [HELD, HELD],
            out_specs=[
                pl.BlockSpec((count, BLOCK), lambda j, s: (0, j)),
                pl.BlockSpec((8, count), lambda j, s: (0, 0)),
            ],
            scratch_shapes=logits_scratch(count, width),
        ),
        out_shape=[
            jax.ShapeDtypeStruct((count, words), F32),
            jax.ShapeDtypeStruct((8, count), F32),
        ],
        compiler_params=pltpu.CompilerParams(vmem_limit_bytes=40 << 20),
        cost_estimate=pl.CostEstimate(
            flops=2 * count * words * width, transcendentals=count * words, bytes_accessed=12 << 20
        ),
        name="draft_logits",
    )(place, *rows, own, other)


def teacher_kernel(place, *refs):
    p_refs, q_refs = refs[0:4], refs[4:8]
    own_ref, other_ref, draft_stats, out_ref, stats_ref = refs[8:13]
    x_ref, held_ref, arrived, top_ref, sum_ref = refs[13:]
    slot = fetch_words(own_ref, other_ref, held_ref, arrived)

    @pl.when(pl.program_id(0) == 0)
    def _():
        cut = p_refs[0].shape[-1]
        for k in range(4):
            for i in range(4):
                for j in range(4):
                    row = place[k] + place[4 + i] + place[8 + j]
                    x_ref[pl.ds(pl.multiple_of(row, 16), 16), :cut] = p_refs[k][i, j]
                    row = place[8 + k] + place[4 + i] + place[j]
                    x_ref[pl.ds(pl.multiple_of(row, 16), 16), cut:] = q_refs[k][i, j]

    logits_step(slot, x_ref, held_ref, out_ref, top_ref, sum_ref)

    @pl.when(pl.program_id(0) == pl.num_programs(0) - 1)
    def _():
        teacher = totals_rows(top_ref, sum_ref)
        stats_ref[...] = jnp.concatenate([teacher[0:2], draft_stats[0:2], teacher[4:8]], axis=0)


def teacher_logits(place, parts, own, other, draft_stats):
    words, width = 2 * own.shape[0], own.shape[1]
    count = 1024
    whole = [
        pl.BlockSpec(p.shape, lambda j, s: (0, 0, 0, 0), pipeline_mode=pl.Buffered(1))
        for p in parts
    ]
    return pl.pallas_call(
        teacher_kernel,
        grid_spec=pltpu.PrefetchScalarGridSpec(
            num_scalar_prefetch=1,
            grid=(words // BLOCK,),
            in_specs=whole + [HELD, HELD, pl.BlockSpec((8, count), lambda j, s: (0, 0))],
            out_specs=[
                pl.BlockSpec((count, BLOCK), lambda j, s: (0, j)),
                pl.BlockSpec((8, count), lambda j, s: (0, 0)),
            ],
            scratch_shapes=logits_scratch(count, width),
        ),
        out_shape=[
            jax.ShapeDtypeStruct((count, words), F32),
            jax.ShapeDtypeStruct((8, count), F32),
        ],
        compiler_params=pltpu.CompilerParams(vmem_limit_bytes=48 << 20),
        cost_estimate=pl.CostEstimate(
            flops=2 * count * words * width, transcendentals=count * words, bytes_accessed=20 << 20
        ),
        name="teacher_logits",
    )(place, *parts, own, other, draft_stats)


def gradient_kernel(starts, teacher_ref, draft_ref, rows_ref, own_ref, other_ref, out_ref, delta_ref):
    count, words = teacher_ref.shape
    column = jnp.transpose(jnp.concatenate([rows_ref[...]] * 16, axis=0))
    half = words // 2
    lane = lax.broadcasted_iota(jnp.int32, (count, half), 1)
    wanted = column[:, 4:5].astype(jnp.int32)
    for h in range(2):
        at = slice(h * half, (h + 1) * half)
        teacher = jnp.exp(teacher_ref[:, at] - column[:, 0:1]) * column[:, 1:2]
        draft = jnp.exp(draft_ref[:, at] - column[:, 2:3]) * column[:, 3:4]
        soft = teacher + jnp.where(lane + starts[h] == wanted, MIXING, 0.0)
        delta_ref[:, at] = (draft - soft).astype(BF16)
    total = jnp.dot(delta_ref[:, :half], own_ref[...], preferred_element_type=F32)
    total = total + jnp.dot(delta_ref[:, half:], other_ref[...], preferred_element_type=F32)
    total = total.astype(BF16)
    for f in range(8):
        for t in range(8):
            out_ref[t, f, 0] = total[t * 32 : t * 32 + 32, f * 256 : f * 256 + 256]


def gradient_parts(starts, teacher, draft, rows, own, other):
    count, words = teacher.shape
    width = own.shape[1]
    tile = 256
    held = pl.BlockSpec(own.shape, lambda j, s: (0, 0), pipeline_mode=pl.Buffered(1))
    return pl.pallas_call(
        gradient_kernel,
        grid_spec=pltpu.PrefetchScalarGridSpec(
            num_scalar_prefetch=1,
            grid=(count // tile,),
            in_specs=[
                pl.BlockSpec((tile, words), lambda j, s: (j, 0)),
                pl.BlockSpec((tile, words), lambda j, s: (j, 0)),
                pl.BlockSpec((8, tile), lambda j, s: (0, j)),
                held,
                held,
            ],
            out_specs=pl.BlockSpec((8, 8, 1, 32, 256), lambda j, s: (0, 0, j, 0, 0)),
            scratch_shapes=[pltpu.VMEM((tile, words), BF16)],
        ),
        out_shape=jax.ShapeDtypeStruct((8, 8, 4, 32, 256), BF16),
        compiler_params=pltpu.CompilerParams(vmem_limit_bytes=40 << 20),
        cost_estimate=pl.CostEstimate(
            flops=2 * count * words * width, transcendentals=2 * count * words, bytes_accessed=16 << 20
        ),
        name="gradient_parts",
    )(starts, teacher, draft, rows, own, other)


def on_device(
    hidden_in,
    attn_gain,
    w_query,
    w_key,
    w_value,
    w_out,
    final_gain,
    teacher_head,
    draft_rows,
    draft_head,
    target_ids,
    rollout_lengths,
    stretch_order,
):
    row_count = hidden_in.shape[0]
    head_dim = HEAD_DIM
    local_heads = w_query.shape[1] // head_dim
    local_groups = w_key.shape[1] // head_dim
    group_size = local_heads // local_groups
    half_rows = row_count // 2
    stretch_ids = jnp.arange(stretch_order.shape[0], dtype=jnp.int32)
    rollout_ends = jnp.cumsum(rollout_lengths)
    my_x, my_yh, my_yl = lax.axis_index("x"), lax.axis_index("yh"), lax.axis_index("yl")
    my_z, my_c = lax.axis_index("z"), lax.axis_index("c")

    def locate(row_ids):
        stretch_hit = (row_ids // half_rows)[:, None] == stretch_ids[None, :]
        stretch_start = jnp.sum(jnp.where(stretch_hit, stretch_order[None, :], 0), axis=1)
        positions = stretch_start * half_rows + row_ids % half_rows
        rollouts = jnp.sum((positions[:, None] >= rollout_ends[None, :]).astype(jnp.int32), axis=1)
        return (positions, rollouts)

    lines = jnp.arange(row_count, dtype=jnp.int32)
    query_pos, query_roll = locate(lax.axis_index(CTX) * row_count + lines)
    normed = rms_scale(hidden_in.astype(F32), attn_gain).astype(BF16)
    keys = jnp.dot(normed, w_key, preferred_element_type=F32).reshape(
        row_count, local_groups, head_dim
    )
    keys = rotate(keys, query_pos).astype(BF16).reshape(row_count, local_groups * head_dim)
    values = jnp.dot(normed, w_value, preferred_element_type=F32).astype(BF16)
    both = jnp.concatenate([keys, values], axis=1)
    copies = jnp.broadcast_to(both[None], (8, *both.shape))
    both = lax.all_to_all(copies, ("yh", "z"), split_axis=0, concat_axis=0, tiled=True)
    both = both.reshape(8 * row_count, -1)
    both = ring(both, C)
    both = jnp.concatenate(both, axis=0)
    key_width = local_groups * head_dim
    key_piece = both[:, :key_width].reshape(-1, local_groups, head_dim)
    value_piece = both[:, key_width:].reshape(-1, local_groups, head_dim)

    queries = jnp.dot(normed, w_query, preferred_element_type=F32).reshape(
        row_count, local_heads, head_dim
    )
    queries = (
        rotate(queries, query_pos)
        .astype(BF16)
        .reshape(row_count, local_groups, group_size, head_dim)
    )
    slots = jnp.arange(key_piece.shape[0], dtype=jnp.int32)
    slot = slots // row_count
    from_c = (my_c + slot // 8) % 2
    owner = slot % 8 * 2 + from_c
    key_pos, key_roll = locate(owner * row_count + slots % row_count)
    allowed = (key_pos[None, :] <= query_pos[:, None]) & (key_roll[None, :] == query_roll[:, None])
    visible = allowed[:, None, None, :]
    scores = jnp.einsum(
        "tkgd,nkd->tkgn", queries, key_piece, preferred_element_type=F32
    ) * head_dim ** (-0.5)
    scores = jnp.where(visible, scores, NEGATIVE)
    top = jnp.max(scores, axis=-1)
    weights = jnp.where(visible, jnp.exp(scores - top[..., None]), 0.0)
    weight_sum = jnp.sum(weights, axis=-1)
    weighted = jnp.einsum(
        "tkgn,nkd->tkgd", weights.astype(BF16), value_piece, preferred_element_type=F32
    )
    attended = (
        (weighted / weight_sum[..., None]).astype(BF16).reshape(row_count, local_heads * head_dim)
    )

    partial_value = jnp.dot(attended, w_out, preferred_element_type=F32).astype(BF16)
    shares = lax.axis_size(VOCAB)
    share_rows = row_count // shares
    arrived = lax.all_to_all(
        partial_value.reshape(shares, share_rows, -1),
        VOCAB,
        split_axis=0,
        concat_axis=0,
        tiled=True,
    )
    own_rows = lax.dynamic_slice_in_dim(
        hidden_in, lax.axis_index(VOCAB) * share_rows, share_rows, 0
    )
    mixed = own_rows.astype(F32) + jnp.sum(arrived.astype(F32), axis=0)
    final = rms_scale(mixed, final_gain).astype(BF16)

    teacher_other = shifted(teacher_head, C, 1)
    draft_other = shifted(draft_head, C, 1)

    turns = jnp.arange(4, dtype=jnp.int32)
    at_x, at_z = (my_x + turns) % 4 * 256, (my_z + turns) % 4 * 32
    at_y = (my_yh * 2 + my_yl + turns) % 4
    at_y = at_y // 2 * 128 + at_y % 2 * 16
    even = my_c == 0
    place = jnp.concatenate(
        [
            jnp.where(even, at_x, at_y),
            jnp.where(even, at_y, at_x),
            at_z,
            (my_yh + turns) % 2 * 128,
        ]
    )
    here = draft_rows.reshape(4, 2 * share_rows, -1)
    there = shifted(here, ("yh",), 1)
    ahead, behind = shifted(here, Z, 3), shifted(here, Z, 1)
    ahead_there, behind_there = shifted(there, Z, 3), shifted(there, Z, 1)
    far, far_there = shifted(ahead, Z, 3), shifted(behind_there, Z, 1)
    draft_part, draft_stats = draft_logits(
        place,
        [here, ahead, far, behind, there, ahead_there, far_there, behind_there],
        draft_head,
        draft_other,
    )

    p, q = jnp.split(final, [2560], axis=1)
    p = spread(p, "zz")
    q = spread(q, "xy")
    p, q = jnp.stack(p), jnp.stack(q)
    p = spread(p, "yx")
    q = spread(q, "yx")
    p, q = jnp.stack(p), jnp.stack(q)
    p = spread(p, "xy")
    q = spread(q, "zz")
    teacher_part, stats = teacher_logits(place, p + q, teacher_head, teacher_other, draft_stats)

    def merged(pieces):
        tops = jnp.max(pieces[:, 0::2], axis=0)
        sums = jnp.sum(pieces[:, 1::2] * jnp.exp(pieces[:, 0::2] - tops), axis=0)
        return jnp.stack([tops[0], sums[0], tops[1], sums[1]])

    for axes in (("x", "yl"), ("yh", "z")):
        copies = jnp.broadcast_to(stats[None, :4], (8, *stats[:4].shape))
        stats = merged(lax.all_to_all(copies, axes, split_axis=0, concat_axis=0, tiled=True))
    targets = target_ids.reshape(2, 4, 2, 4, 2 * share_rows)
    targets = lax.dynamic_index_in_dim(targets, my_c, 2, keepdims=False)
    targets = jnp.transpose(targets, (2, 0, 1, 3)).reshape(-1).astype(F32)
    nothing = jnp.zeros_like(targets)
    rows = jnp.stack(
        [
            stats[0],
            (1.0 - MIXING) / stats[1],
            stats[2],
            1.0 / stats[3],
            targets,
            nothing,
            nothing,
            nothing,
        ]
    )
    word_count = teacher_head.shape[0]
    block_id = lax.axis_index(VOCAB) * lax.axis_size(CTX) + (my_yh * 4 + my_z) * 2
    starts = jnp.stack([block_id + my_c, block_id + 1 - my_c]).astype(jnp.int32) * word_count
    parts = gradient_parts(starts, teacher_part, draft_part, rows, draft_head, draft_other)
    parts = parts.reshape(64, row_count, -1)
    arrived = lax.all_to_all(parts, CHIPS, split_axis=0, concat_axis=0, tiled=True)
    return jnp.sum(arrived.astype(F32), axis=0)


def solution(mesh):
    torus = Mesh(mesh.devices.reshape(2, 4, 2, 4, 2), ("yh", "z", "c", "x", "yl"))
    words = P(("x", "yl", "yh", "z", "c"), None)

    return jax.shard_map(
        on_device,
        mesh=torus,
        in_specs=(
            P(CTX, None),
            P(),
            P(None, VOCAB),
            P(None, VOCAB),
            P(None, VOCAB),
            P(VOCAB, None),
            P(),
            words,
            P(CTX, None),
            words,
            P(),
            P(),
            P(),
        ),
        out_specs=P(CTX, VOCAB),
        check_vma=False,
    )
```

```python
import jax
import jax.numpy as jnp
from jax import lax
from jax.experimental import pallas as pl
from jax.experimental.pallas import tpu as pltpu
from jax.sharding import Mesh
from jax.sharding import PartitionSpec as P


HEAD_DIM = 128
EPSILON = 1e-05
ROPE_BASE = 500000.0
MIXING = 0.5
NEGATIVE = -1e30

CTX = ("yh", "z", "c")
VOCAB = ("x", "yl")
X, Y, Z, C = ("x",), ("yh", "yl"), ("z",), ("c",)
CHIPS = ("yh", "z", "x", "yl")
F32, BF16 = jnp.float32, jnp.bfloat16


def shifted(a, axes, k):
    n = lax.axis_size(axes)
    return lax.ppermute(a, axes, [(i, (i + k) % n) for i in range(n)])


def ring(a, axes):
    n = lax.axis_size(axes)
    return [a] + [shifted(a, axes, n - d) for d in range(1, n)]


EVERY = ("yh", "z", "c", "x", "yl")


def moved(a, along, k):
    pairs = []
    for source in range(128):
        yh, z, c = source // 64, source // 16 % 4, source // 8 % 2
        x, yl = source // 2 % 4, source % 2
        y = 2 * yh + yl
        x = (x + k) % 4 if along[c] == "x" else x
        y = (y + k) % 4 if along[c] == "y" else y
        z = (z + k) % 4 if along[c] == "z" else z
        pairs.append((source, (((y // 2 * 4 + z) * 2 + c) * 4 + x) * 2 + y % 2))
    return lax.ppermute(a, EVERY, pairs)


def spread(a, along):
    return [a] + [moved(a, along, 4 - d) for d in range(1, 4)]


def rms_scale(values, gain):
    mean_square = jnp.mean(values * values, axis=-1, keepdims=True)
    return values * lax.rsqrt(mean_square + EPSILON) * gain


def rotate(vectors, positions):
    half_dim = vectors.shape[-1] // 2
    exponents = jnp.arange(half_dim, dtype=F32) * (2.0 / vectors.shape[-1])
    frequencies = jnp.power(ROPE_BASE, -exponents)
    angles = positions.astype(F32)[:, None] * frequencies[None, :]
    cosine_values = jnp.cos(angles)[:, None, :]
    sine_values = jnp.sin(angles)[:, None, :]
    leading = vectors[..., :half_dim]
    trailing = vectors[..., half_dim:]
    return jnp.concatenate(
        [
            leading * cosine_values - trailing * sine_values,
            trailing * cosine_values + leading * sine_values,
        ],
        axis=-1,
    )


NT = (((1,), (1,)), ((), ()))


BLOCK = 256


def fetch_words(own_ref, other_ref, held_ref, arrived):
    j, steps = pl.program_id(0), pl.num_programs(0)
    half = steps // 2

    def start(step, slot):
        @pl.when(step < half)
        def _():
            at = pl.ds(pl.multiple_of(step * BLOCK, BLOCK), BLOCK)
            pltpu.make_async_copy(own_ref.at[at], held_ref.at[slot], arrived.at[slot]).start()

        @pl.when(step >= half)
        def _():
            at = pl.ds(pl.multiple_of((step - half) * BLOCK, BLOCK), BLOCK)
            pltpu.make_async_copy(other_ref.at[at], held_ref.at[slot], arrived.at[slot]).start()

    @pl.when(j == 0)
    def _():
        start(0, 0)

    @pl.when(j + 1 < steps)
    def _():
        start(j + 1, (j + 1) % 2)

    slot = j % 2
    pltpu.make_async_copy(own_ref.at[pl.ds(0, BLOCK)], held_ref.at[slot], arrived.at[slot]).wait()
    return slot


def logits_step(slot, x_ref, held_ref, out_ref, top_ref, sum_ref):
    @pl.when(pl.program_id(0) == 0)
    def _():
        top_ref[...] = jnp.full_like(top_ref, NEGATIVE)
        sum_ref[...] = jnp.zeros_like(sum_ref)

    part = lax.dot_general(x_ref[...], held_ref[slot], NT, preferred_element_type=F32)
    out_ref[...] = part
    pieces = [part[:, k : k + 128] for k in range(0, BLOCK, 128)]
    old = top_ref[...]
    new = old
    for piece in pieces:
        new = jnp.maximum(new, piece)
    total = sum_ref[...] * jnp.exp(old - new)
    for piece in pieces:
        total = total + jnp.exp(piece - new)
    sum_ref[...] = total
    top_ref[...] = new


def totals_rows(top_ref, sum_ref):
    shape = top_ref.shape
    lanes = top_ref[...]
    top = jnp.max(lanes, axis=1, keepdims=True)
    total = jnp.sum(sum_ref[...] * jnp.exp(lanes - top), axis=1, keepdims=True)
    lane = lax.broadcasted_iota(jnp.int32, shape, 1)
    both = jnp.where(lane == 0, jnp.broadcast_to(top, shape), jnp.broadcast_to(total, shape))
    return jnp.transpose(both)


HELD = pl.BlockSpec(memory_space=pltpu.HBM)


def logits_scratch(count, width):
    return [
        pltpu.VMEM((count, width), BF16),
        pltpu.VMEM((2, BLOCK, width), BF16),
        pltpu.SemaphoreType.DMA((2,)),
        pltpu.VMEM((count, 128), F32),
        pltpu.VMEM((count, 128), F32),
    ]


def draft_kernel(place, *refs):
    row_refs = refs[0:8]
    own_ref, other_ref, out_ref, stats_ref, x_ref, held_ref, arrived, top_ref, sum_ref = refs[8:]
    slot = fetch_words(own_ref, other_ref, held_ref, arrived)

    @pl.when(pl.program_id(0) == 0)
    def _():
        for dyh in range(2):
            for dz in range(4):
                base = place[12 + dyh] + place[8 + dz]
                for x in range(4):
                    at = pl.ds(pl.multiple_of(base + x * 256, 32), 32)
                    x_ref[at, :] = row_refs[dyh * 4 + dz][x]

    logits_step(slot, x_ref, held_ref, out_ref, top_ref, sum_ref)

    @pl.when(pl.program_id(0) == pl.num_programs(0) - 1)
    def _():
        stats_ref[...] = totals_rows(top_ref, sum_ref)[:8]


def draft_logits(place, rows, own, other):
    words, width = 2 * own.shape[0], own.shape[1]
    count = 1024
    return pl.pallas_call(
        draft_kernel,
        grid_spec=pltpu.PrefetchScalarGridSpec(
            num_scalar_prefetch=1,
            grid=(words // BLOCK,),
            in_specs=[
                pl.BlockSpec(r.shape, lambda j, s, n=r.ndim: (0,) * n, pipeline_mode=pl.Buffered(1))
                for r in rows
            ]
            + [HELD, HELD],
            out_specs=[
                pl.BlockSpec((count, BLOCK), lambda j, s: (0, j)),
                pl.BlockSpec((8, count), lambda j, s: (0, 0)),
            ],
            scratch_shapes=logits_scratch(count, width),
        ),
        out_shape=[
            jax.ShapeDtypeStruct((count, words), F32),
            jax.ShapeDtypeStruct((8, count), F32),
        ],
        compiler_params=pltpu.CompilerParams(vmem_limit_bytes=40 << 20),
        cost_estimate=pl.CostEstimate(
            flops=2 * count * words * width, transcendentals=count * words, bytes_accessed=12 << 20
        ),
        name="draft_logits",
    )(place, *rows, own, other)


def teacher_kernel(place, *refs):
    p_refs, q_refs = refs[0:4], refs[4:8]
    own_ref, other_ref, draft_stats, out_ref, stats_ref = refs[8:13]
    x_ref, held_ref, arrived, top_ref, sum_ref = refs[13:]
    slot = fetch_words(own_ref, other_ref, held_ref, arrived)

    @pl.when(pl.program_id(0) == 0)
    def _():
        cut = p_refs[0].shape[-1]
        for k in range(4):
            for i in range(4):
                for j in range(4):
                    row = place[k] + place[4 + i] + place[8 + j]
                    x_ref[pl.ds(pl.multiple_of(row, 16), 16), :cut] = p_refs[k][i, j]
                    row = place[8 + k] + place[4 + i] + place[j]
                    x_ref[pl.ds(pl.multiple_of(row, 16), 16), cut:] = q_refs[k][i, j]

    logits_step(slot, x_ref, held_ref, out_ref, top_ref, sum_ref)

    @pl.when(pl.program_id(0) == pl.num_programs(0) - 1)
    def _():
        teacher = totals_rows(top_ref, sum_ref)
        stats_ref[...] = jnp.concatenate([teacher[0:2], draft_stats[0:2]], axis=0)


def teacher_logits(place, parts, own, other, draft_stats):
    words, width = 2 * own.shape[0], own.shape[1]
    count = 1024
    whole = [
        pl.BlockSpec(p.shape, lambda j, s: (0, 0, 0, 0), pipeline_mode=pl.Buffered(1))
        for p in parts
    ]
    return pl.pallas_call(
        teacher_kernel,
        grid_spec=pltpu.PrefetchScalarGridSpec(
            num_scalar_prefetch=1,
            grid=(words // BLOCK,),
            in_specs=whole + [HELD, HELD, pl.BlockSpec((8, count), lambda j, s: (0, 0))],
            out_specs=[
                pl.BlockSpec((count, BLOCK), lambda j, s: (0, j)),
                pl.BlockSpec((4, count), lambda j, s: (0, 0)),
            ],
            scratch_shapes=logits_scratch(count, width),
        ),
        out_shape=[
            jax.ShapeDtypeStruct((count, words), F32),
            jax.ShapeDtypeStruct((4, count), F32),
        ],
        compiler_params=pltpu.CompilerParams(vmem_limit_bytes=48 << 20),
        cost_estimate=pl.CostEstimate(
            flops=2 * count * words * width, transcendentals=count * words, bytes_accessed=20 << 20
        ),
        name="teacher_logits",
    )(place, *parts, own, other, draft_stats)


def gradient_kernel(starts, teacher_ref, draft_ref, rows_ref, own_ref, other_ref, out_ref, delta_ref):
    count, words = teacher_ref.shape
    column = jnp.transpose(jnp.concatenate([rows_ref[...]] * 16, axis=0))
    half = words // 2
    lane = lax.broadcasted_iota(jnp.int32, (count, half), 1)
    wanted = column[:, 4:5].astype(jnp.int32)
    for h in range(2):
        at = slice(h * half, (h + 1) * half)
        teacher = jnp.exp(teacher_ref[:, at] - column[:, 0:1]) * column[:, 1:2]
        draft = jnp.exp(draft_ref[:, at] - column[:, 2:3]) * column[:, 3:4]
        soft = teacher + jnp.where(lane + starts[h] == wanted, MIXING, 0.0)
        delta_ref[:, at] = (draft - soft).astype(BF16)
    total = jnp.dot(delta_ref[:, :half], own_ref[...], preferred_element_type=F32)
    total = total + jnp.dot(delta_ref[:, half:], other_ref[...], preferred_element_type=F32)
    total = total.astype(BF16)
    for f in range(8):
        for t in range(8):
            out_ref[t, f, 0] = total[t * 32 : t * 32 + 32, f * 256 : f * 256 + 256]


def gradient_parts(starts, teacher, draft, rows, own, other):
    count, words = teacher.shape
    width = own.shape[1]
    tile = 256
    held = pl.BlockSpec(own.shape, lambda j, s: (0, 0), pipeline_mode=pl.Buffered(1))
    return pl.pallas_call(
        gradient_kernel,
        grid_spec=pltpu.PrefetchScalarGridSpec(
            num_scalar_prefetch=1,
            grid=(count // tile,),
            in_specs=[
                pl.BlockSpec((tile, words), lambda j, s: (j, 0)),
                pl.BlockSpec((tile, words), lambda j, s: (j, 0)),
                pl.BlockSpec((8, tile), lambda j, s: (0, j)),
                held,
                held,
            ],
            out_specs=pl.BlockSpec((8, 8, 1, 32, 256), lambda j, s: (0, 0, j, 0, 0)),
            scratch_shapes=[pltpu.VMEM((tile, words), BF16)],
        ),
        out_shape=jax.ShapeDtypeStruct((8, 8, 4, 32, 256), BF16),
        compiler_params=pltpu.CompilerParams(vmem_limit_bytes=40 << 20),
        cost_estimate=pl.CostEstimate(
            flops=2 * count * words * width, transcendentals=2 * count * words, bytes_accessed=16 << 20
        ),
        name="gradient_parts",
    )(starts, teacher, draft, rows, own, other)


def keys_kernel(hidden_from, key_from, value_from, gain_ref, cosine_ref, sine_ref, *refs):
    normed_ref, copies_ref, hidden_ref, key_ref, value_ref, arrived = refs
    fetches = [
        pltpu.make_async_copy(hidden_from, hidden_ref, arrived.at[0]),
        pltpu.make_async_copy(key_from, key_ref, arrived.at[1]),
        pltpu.make_async_copy(value_from, value_ref, arrived.at[2]),
    ]
    for fetch in fetches:
        fetch.start()
    fetches[0].wait()
    values = hidden_ref[...].astype(F32)
    mean_square = jnp.mean(values * values, axis=-1, keepdims=True)
    normed = (values * lax.rsqrt(mean_square + EPSILON) * gain_ref[...]).astype(BF16)
    normed_ref[...] = normed
    fetches[1].wait()
    keys = jnp.dot(normed, key_ref[...], preferred_element_type=F32)
    turned = keys * cosine_ref[...] + pltpu.roll(keys, HEAD_DIM // 2, 1) * sine_ref[...]
    fetches[2].wait()
    passed = jnp.dot(normed, value_ref[...], preferred_element_type=F32)
    both = jnp.concatenate([turned.astype(BF16), passed.astype(BF16)], axis=1)
    for k in range(copies_ref.shape[0]):
        copies_ref[k] = both


def keys_and_values(hidden, gain, w_key, w_value, cosine, sine, copies):
    rows, width = hidden.shape
    large = [pltpu.with_memory_space_constraint(a, pltpu.HBM) for a in (hidden, w_key, w_value)]
    whole = pl.BlockSpec(memory_space=pltpu.VMEM)
    return pl.pallas_call(
        keys_kernel,
        in_specs=[HELD] * 3 + [whole] * 3,
        out_shape=[
            jax.ShapeDtypeStruct((rows, width), BF16),
            jax.ShapeDtypeStruct((copies, rows, 2 * HEAD_DIM), BF16),
        ],
        scratch_shapes=[pltpu.VMEM(a.shape, BF16) for a in large]
        + [pltpu.SemaphoreType.DMA((3,))],
        compiler_params=pltpu.CompilerParams(vmem_limit_bytes=24 << 20),
        cost_estimate=pl.CostEstimate(
            flops=4 * rows * width * HEAD_DIM, transcendentals=rows, bytes_accessed=5 << 20
        ),
        name="keys_and_values",
    )(*large, gain[None, :], cosine, sine)


def on_device(
    hidden_in,
    attn_gain,
    w_query,
    w_key,
    w_value,
    w_out,
    final_gain,
    teacher_head,
    draft_rows,
    draft_head,
    target_ids,
    rollout_lengths,
    stretch_order,
):
    row_count = hidden_in.shape[0]
    head_dim = HEAD_DIM
    local_heads = w_query.shape[1] // head_dim
    local_groups = w_key.shape[1] // head_dim
    group_size = local_heads // local_groups
    half_rows = row_count // 2
    stretch_ids = jnp.arange(stretch_order.shape[0], dtype=jnp.int32)
    rollout_ends = jnp.cumsum(rollout_lengths)
    my_x, my_yh, my_yl = lax.axis_index("x"), lax.axis_index("yh"), lax.axis_index("yl")
    my_z, my_c = lax.axis_index("z"), lax.axis_index("c")

    def locate(row_ids):
        stretch_hit = (row_ids // half_rows)[:, None] == stretch_ids[None, :]
        stretch_start = jnp.sum(jnp.where(stretch_hit, stretch_order[None, :], 0), axis=1)
        positions = stretch_start * half_rows + row_ids % half_rows
        rollouts = jnp.sum((positions[:, None] >= rollout_ends[None, :]).astype(jnp.int32), axis=1)
        return (positions, rollouts)

    lines = jnp.arange(row_count, dtype=jnp.int32)
    query_pos, query_roll = locate(lax.axis_index(CTX) * row_count + lines)
    exponents = jnp.arange(head_dim // 2, dtype=F32) * (2.0 / head_dim)
    angles = query_pos.astype(F32)[:, None] * jnp.power(ROPE_BASE, -exponents)[None, :]
    cosine, sine = jnp.cos(angles), jnp.sin(angles)
    normed, copies = keys_and_values(
        hidden_in,
        attn_gain,
        w_key,
        w_value,
        jnp.concatenate([cosine, cosine], axis=1),
        jnp.concatenate([-sine, sine], axis=1),
        8,
    )
    both = lax.all_to_all(copies, ("yh", "z"), split_axis=0, concat_axis=0, tiled=True)
    both = both.reshape(8 * row_count, -1)
    both = ring(both, C)
    both = jnp.concatenate(both, axis=0)
    key_width = local_groups * head_dim
    key_piece = both[:, :key_width].reshape(-1, local_groups, head_dim)
    value_piece = both[:, key_width:].reshape(-1, local_groups, head_dim)

    queries = jnp.dot(normed, w_query, preferred_element_type=F32).reshape(
        row_count, local_heads, head_dim
    )
    queries = (
        rotate(queries, query_pos)
        .astype(BF16)
        .reshape(row_count, local_groups, group_size, head_dim)
    )
    slots = jnp.arange(key_piece.shape[0], dtype=jnp.int32)
    slot = slots // row_count
    from_c = (my_c + slot // 8) % 2
    owner = slot % 8 * 2 + from_c
    key_pos, key_roll = locate(owner * row_count + slots % row_count)
    allowed = (key_pos[None, :] <= query_pos[:, None]) & (key_roll[None, :] == query_roll[:, None])
    visible = allowed[:, None, None, :]
    scores = jnp.einsum(
        "tkgd,nkd->tkgn", queries, key_piece, preferred_element_type=F32
    ) * head_dim ** (-0.5)
    scores = jnp.where(visible, scores, NEGATIVE)
    top = jnp.max(scores, axis=-1)
    weights = jnp.where(visible, jnp.exp(scores - top[..., None]), 0.0)
    weight_sum = jnp.sum(weights, axis=-1)
    weighted = jnp.einsum(
        "tkgn,nkd->tkgd", weights.astype(BF16), value_piece, preferred_element_type=F32
    )
    attended = (
        (weighted / weight_sum[..., None]).astype(BF16).reshape(row_count, local_heads * head_dim)
    )

    partial_value = jnp.dot(attended, w_out, preferred_element_type=F32).astype(BF16)
    shares = lax.axis_size(VOCAB)
    share_rows = row_count // shares
    arrived = lax.all_to_all(
        partial_value.reshape(shares, share_rows, -1),
        VOCAB,
        split_axis=0,
        concat_axis=0,
        tiled=True,
    )
    own_rows = lax.dynamic_slice_in_dim(
        hidden_in, lax.axis_index(VOCAB) * share_rows, share_rows, 0
    )
    mixed = own_rows.astype(F32) + jnp.sum(arrived.astype(F32), axis=0)
    final = rms_scale(mixed, final_gain).astype(BF16)

    teacher_other = shifted(teacher_head, C, 1)
    draft_other = shifted(draft_head, C, 1)

    turns = jnp.arange(4, dtype=jnp.int32)
    at_x, at_z = (my_x + turns) % 4 * 256, (my_z + turns) % 4 * 32
    at_y = (my_yh * 2 + my_yl + turns) % 4
    at_y = at_y // 2 * 128 + at_y % 2 * 16
    even = my_c == 0
    place = jnp.concatenate(
        [
            jnp.where(even, at_x, at_y),
            jnp.where(even, at_y, at_x),
            at_z,
            (my_yh + turns) % 2 * 128,
        ]
    )
    here = draft_rows.reshape(4, 2 * share_rows, -1)
    there = shifted(here, ("yh",), 1)
    ahead, behind = shifted(here, Z, 3), shifted(here, Z, 1)
    ahead_there, behind_there = shifted(there, Z, 3), shifted(there, Z, 1)
    far, far_there = shifted(ahead, Z, 3), shifted(behind_there, Z, 1)
    draft_part, draft_stats = draft_logits(
        place,
        [here, ahead, far, behind, there, ahead_there, far_there, behind_there],
        draft_head,
        draft_other,
    )

    p, q = jnp.split(final, [2560], axis=1)
    p = spread(p, "zz")
    q = spread(q, "xy")
    p, q = jnp.stack(p), jnp.stack(q)
    p = spread(p, "yx")
    q = spread(q, "yx")
    p, q = jnp.stack(p), jnp.stack(q)
    p = spread(p, "xy")
    q = spread(q, "zz")
    teacher_part, stats = teacher_logits(place, p + q, teacher_head, teacher_other, draft_stats)

    def merged(pieces):
        tops = jnp.max(pieces[:, 0::2], axis=0)
        sums = jnp.sum(pieces[:, 1::2] * jnp.exp(pieces[:, 0::2] - tops), axis=0)
        return jnp.stack([tops[0], sums[0], tops[1], sums[1]])

    for axes in (X, Y, Z):
        stats = merged(jnp.stack(ring(stats, axes)))
    targets = target_ids.reshape(2, 4, 2, 4, 2 * share_rows)
    targets = lax.dynamic_index_in_dim(targets, my_c, 2, keepdims=False)
    targets = jnp.transpose(targets, (2, 0, 1, 3)).reshape(-1).astype(F32)
    nothing = jnp.zeros_like(targets)
    rows = jnp.stack(
        [
            stats[0],
            (1.0 - MIXING) / stats[1],
            stats[2],
            1.0 / stats[3],
            targets,
            nothing,
            nothing,
            nothing,
        ]
    )
    word_count = teacher_head.shape[0]
    block_id = lax.axis_index(VOCAB) * lax.axis_size(CTX) + (my_yh * 4 + my_z) * 2
    starts = jnp.stack([block_id + my_c, block_id + 1 - my_c]).astype(jnp.int32) * word_count
    parts = gradient_parts(starts, teacher_part, draft_part, rows, draft_head, draft_other)
    parts = parts.reshape(64, row_count, -1)
    arrived = lax.all_to_all(parts, CHIPS, split_axis=0, concat_axis=0, tiled=True)
    return jnp.sum(arrived.astype(F32), axis=0)


def solution(mesh):
    torus = Mesh(mesh.devices.reshape(2, 4, 2, 4, 2), ("yh", "z", "c", "x", "yl"))
    words = P(("x", "yl", "yh", "z", "c"), None)

    return jax.shard_map(
        on_device,
        mesh=torus,
        in_specs=(
            P(CTX, None),
            P(),
            P(None, VOCAB),
            P(None, VOCAB),
            P(None, VOCAB),
            P(VOCAB, None),
            P(),
            words,
            P(CTX, None),
            words,
            P(),
            P(),
            P(),
        ),
        out_specs=P(CTX, VOCAB),
        check_vma=False,
    )
```
